128 devices in a mesh: group: 8 (over x, core), ctx: 16 (over y, z).
Axes of the slice: x: 4, y: 4, z: 4, core: 2. Of those that a mesh axis runs over, the one named last changes fastest.
Arguments:
- query_rows: bfloat16 [8, 4096, 4096], P('group', 'ctx'), may hold values from -250 to 250
- key_rows: bfloat16 [8, 4096, 512], P('group', 'ctx'), may hold values from -7 to 7
- value_rows: bfloat16 [8, 4096, 512], P('group', 'ctx'), may hold values from -6 to 6
- documents: int32 [8, 4096], P('group', 'ctx'), may hold values from 0 to 3, never falling along the last dimension, each value on 1 to 2560 neighbouring positions
- owners: int32 [8, 128, 1], P('group', 'ctx'), may hold values from 0 to 7; in each aligned block of 8 rows (0 to 7, 8 to 15, ..., all dimensions but the last counted through in order) at most 2 rows name the same one
Outputs:
- attended: bfloat16 [8, 4096, 4096], P('group', 'ctx')
- page_pool: bfloat16 [8, 256, 2, 128, 128], P('group', 'ctx')
- page_scales: bfloat16 [8, 256, 2], P('group', 'ctx')
The draws below stay inside these ranges and needn't reach their ends.
Inputs may be any that keep to these rules, and one draw needn't show every extreme that they name: `documents`: document numbers never fall along a group's tokens; each document has at most 2560 tokens. `owners`: among the pages of one device, no owner is named more than 2 times.
All inputs are finite; a program needn't handle non-finite values.
Results may differ from the reference program's by a relative error of at most 0.0028.
Values may be sent and summed in bfloat16 or wider, within the bound.
No kernel may reach another device: no remote copies, remote signals or barrier semaphores. Data moves between devices by JAX's collectives and lax.ppermute only.
A program may use at most 128 MiB of HBM per device.

```python
import math
import jax
import jax.numpy as jnp
import numpy as np
from jax import lax

E = 128
HQ = 32
HK = 4
PAGE = 128
TOK_DEV = 256
DOCS = 4
SEQ = 4096
LONGEST = 2560
GROUPS = 8
PAGES = 128
MOST = 2
POOL = 256
N_GROUP = 8
N_CTX = 16


def drawn_pair(key):
    base_key = jax.random.fold_in(key, 7101)
    subkeys = jax.random.split(base_key, 2)
    repeat = HQ // HK
    key_part = jnp.clip(1.6 * jax.random.normal(subkeys[0], (GROUPS, SEQ, HK, E), jnp.float32), -7.0, 7.0)
    query_part = jnp.clip(1.6 * jax.random.normal(subkeys[1], (GROUPS, SEQ, HK, repeat, E), jnp.float32), -7.0, 7.0)
    return (query_part.reshape(GROUPS, SEQ, HQ * E), key_part.reshape(GROUPS, SEQ, HK * E))


def draw_query_rows(key, part):
    return drawn_pair(key)[0].astype(jnp.bfloat16)


def draw_key_rows(key, part):
    return drawn_pair(key)[1].astype(jnp.bfloat16)


def shard_levels(rng, dims, cuts, smallest, high):
    loudness, own = 1.0, jax.random.fold_in(rng, 6)
    for dim, parts in cuts:
        draws = jnp.exp(jax.random.uniform(jax.random.fold_in(own, dim), (parts,), jnp.float32, smallest / len(cuts), high / len(cuts)))
        loudness = loudness * jnp.repeat(draws, dims[dim] // parts).reshape([-1 if axis == dim else 1 for axis in range(len(dims))])
    return loudness


def profile(number_of, total, bound, lean):
    weights = [(1 << 20) // math.isqrt(grade ** lean) + 1 for grade in range(2, number_of + 1)]
    rest, counts = total - bound - (number_of - 1), [1] * (number_of - 1)
    while rest > 0:
        candidates = [i for i in range(number_of - 1) if counts[i] < bound]
        whole, remaining = sum([weights[i] for i in candidates]), rest
        for i in candidates:
            extra = min(bound - counts[i], max(1, remaining * weights[i] // whole), rest)
            counts[i] = counts[i] + extra
            rest = rest - extra
    return np.array([bound] + counts)


def uneven(rng, count, total, bound, skew):
    if count == 2:
        one = jax.random.randint(rng, (), max(1, total - bound), min(bound, total - 1) + 1)
        return jnp.stack([one, total - one])
    tallies = jnp.asarray(profile(count, total, bound, skew), jnp.int32)
    couples = (count - 1) // 2
    source_of, taker = tallies[1:1 + 2 * couples:2], tallies[2:2 + 2 * couples:2]
    margin = jnp.minimum(source_of - 1, bound - taker)
    passed = jax.random.randint(jax.random.fold_in(rng, 1), (couples,), 0, 1 << 20) % (margin + 1)
    tallies = tallies.at[1:1 + 2 * couples:2].set(source_of - passed).at[2:2 + 2 * couples:2].set(taker + passed)
    return tallies[jax.random.permutation(jax.random.fold_in(rng, 2), count)]


def assign_block(own_key, own, number, rows, count, top, most, skew):
    ranking = jax.random.permutation(own_key, count)
    heavy_load, common = shares(count, rows * top, most, skew, True), shares(count, rows * top, most, skew, False)
    places = jnp.arange(count)

    def named(tallies, rotation):
        used = int((tallies > 0).sum())
        fixed = max(1, used // 4)
        moved = fixed + (places - fixed + rotation * (used - fixed)) % max(1, count - fixed)
        return jnp.zeros((count,), jnp.int32).at[ranking[jnp.where(places < fixed, places, moved)]].set(jnp.asarray(tallies, jnp.int32))

    tallies = jnp.where(number % 4 == 0, named(heavy_load, number // 4), named(common, number - number // 4 - 1))
    mixed = jax.random.permutation(jax.random.fold_in(own, 3), count)
    source_of, receiver = mixed[0:count // 2 * 2:2], mixed[1:count // 2 * 2:2]
    room = jnp.minimum(tallies[source_of] - 1, most - tallies[receiver]) // 2
    room = jnp.where((source_of == ranking[0]) | (receiver == ranking[0]) | (tallies[receiver] == 0), 0, jnp.maximum(room, 0))
    moved = jax.random.randint(jax.random.fold_in(own, 4), (count // 2,), 0, 1 << 20) % (room + 1)
    tallies = tallies.at[source_of].add(-moved).at[receiver].add(moved)
    labels = jnp.searchsorted(jnp.cumsum(tallies), jnp.arange(rows * top), side="right").astype(jnp.int32)
    table = labels.reshape(top, rows).T
    table = table[jax.random.permutation(jax.random.fold_in(own, 1), rows)]
    rotation = jax.random.randint(jax.random.fold_in(own, 2), (rows, 1), 0, top)
    return jnp.take_along_axis(table, (jnp.arange(top)[None, :] + rotation) % top, axis=1)


def shares(amount, total, most, skew, full):
    weights = [(1 << 20) // math.isqrt(grade ** skew) + 1 for grade in range(1, amount + 1)]
    largest = most if full else min(most, max(-(-total // amount), total * weights[0] // sum(weights)))
    least = 1 if total - largest >= amount - 1 else 0
    holding, rest = [largest] + [least] * (amount - 1), total - largest - least * (amount - 1)
    while rest > 0:
        candidates = [i for i in range(1, amount) if holding[i] < largest] or [i for i in range(1, amount) if holding[i] < most]
        mass, remaining = sum([weights[i] for i in candidates]), rest
        for i in candidates:
            addition = min(most - holding[i], max(1, remaining * weights[i] // mass), rest)
            holding[i] = holding[i] + addition
            rest = rest - addition
    return np.array(holding)


def centred(key, dims, deviation, bound, cuts=(), kind=jnp.bfloat16):
    array = jax.random.normal(key, dims, jnp.float32) * deviation
    if len(cuts) > 0:
        array = shard_levels(key, dims, cuts, -0.22, 0.18) * array
    return jnp.clip(array, min=-bound, max=bound).astype(kind)


def setup_inputs(seed: int = 0) -> dict:
    key_of = jax.random.split(jax.random.key(seed), 6)
    query_rows = draw_query_rows(jax.random.fold_in(key_of[5], 71), 0)
    key_rows = draw_key_rows(jax.random.fold_in(key_of[5], 71), 0)
    value_rows = centred(key_of[2], (GROUPS, SEQ, HK * E), 1.0, 6.0, ((0, 8), (1, 16)))
    documents = jax.vmap(lambda own: jnp.searchsorted(jnp.cumsum(uneven(own, DOCS, SEQ, LONGEST, 2)), jnp.arange(SEQ), side="right"))(jax.random.split(key_of[3], GROUPS)).reshape((GROUPS, SEQ)).astype(jnp.int32)
    owners_keys = jax.random.split(jax.random.fold_in(key_of[4], 1), GROUPS * PAGES // (TOK_DEV // PAGE * HK))
    owners_turns = jax.random.permutation(jax.random.fold_in(key_of[4], 3), GROUPS * PAGES // (TOK_DEV // PAGE * HK))
    owners = jax.vmap(lambda own, number: assign_block(jax.random.fold_in(key_of[4], 2), own, number, TOK_DEV // PAGE * HK, N_GROUP, 1, MOST, 2))(owners_keys, owners_turns).reshape((GROUPS, PAGES, 1))
    return dict(query_rows=query_rows, key_rows=key_rows, value_rows=value_rows, documents=documents, owners=owners)


epsilon = 1e-06

def attend_group(query_one, key_one, value_one, doc_one):
    repeat = HQ // HK
    score_scale = 1.0 / math.sqrt(E)
    grouped = query_one.reshape(SEQ, HK, repeat, E).astype(jnp.float32)
    key_heads = key_one.reshape(SEQ, HK, E).astype(jnp.float32)
    value_heads = value_one.reshape(SEQ, HK, E).astype(jnp.float32)
    block_rows = math.gcd(SEQ, 512)
    positions = jnp.arange(SEQ, dtype=jnp.int32)

    def one_block(block_index):
        first_row = block_index * block_rows
        query_block = lax.dynamic_slice_in_dim(grouped, first_row, block_rows, 0)
        doc_block = lax.dynamic_slice_in_dim(doc_one, first_row, block_rows, 0)
        query_pos = first_row + jnp.arange(block_rows, dtype=jnp.int32)
        scores = jnp.einsum('qgre,kge->grqk', query_block, key_heads) * score_scale
        visible = (doc_block[:, None] == doc_one[None, :]) & (query_pos[:, None] >= positions[None, :])
        scores = jnp.where(visible, scores, -jnp.inf)
        largest = lax.optimization_barrier(jnp.max(scores, axis=-1, keepdims=True))
        weights = jnp.exp(scores - largest)
        totals = lax.optimization_barrier(jnp.sum(weights, axis=-1))
        rounded = lax.optimization_barrier(weights.astype(jnp.bfloat16)).astype(jnp.float32)
        weighted = jnp.einsum('grqk,kge->qgre', rounded, value_heads)
        result = weighted / jnp.transpose(totals, (2, 0, 1))[..., None]
        return result.astype(jnp.bfloat16)
    blocks = lax.map(one_block, jnp.arange(SEQ // block_rows, dtype=jnp.int32))
    return blocks.reshape(SEQ, HQ * E)

def page_pairs(key_one, value_one):
    block_count = SEQ // PAGE
    key_pages = key_one.reshape(block_count, PAGE, HK, E).transpose(0, 2, 1, 3)
    value_pages = value_one.reshape(block_count, PAGE, HK, E).transpose(0, 2, 1, 3)
    kv_pairs = jnp.stack([key_pages, value_pages], axis=2).reshape(block_count * HK, 2, PAGE, E)
    magnitude = lax.optimization_barrier(jnp.max(jnp.abs(kv_pairs.astype(jnp.float32)), axis=(2, 3))) + epsilon
    scales = magnitude.astype(jnp.bfloat16)
    stored = (kv_pairs.astype(jnp.float32) / scales.astype(jnp.float32)[:, :, None, None]).astype(jnp.bfloat16)
    return (stored, scales)

def reference(query_rows, key_rows, value_rows, documents, owners):
    attended = jnp.stack([attend_group(query_rows[g], key_rows[g], value_rows[g], documents[g]) for g in range(GROUPS)])
    stored, scales = jax.vmap(page_pairs)(key_rows, value_rows)
    per_device = PAGES // N_CTX
    owner_grid = owners[:, :, 0].reshape(GROUPS, N_CTX, per_device)
    page_order = jnp.arange(per_device, dtype=jnp.int32)
    earlier = (owner_grid[..., :, None] == owner_grid[..., None, :]) & (page_order[None, :] < page_order[:, None])
    page_rank = lax.optimization_barrier(jnp.sum(earlier.astype(jnp.int32), axis=-1))
    source = jnp.broadcast_to(jnp.arange(GROUPS, dtype=jnp.int32)[:, None, None], owner_grid.shape)
    column = jnp.broadcast_to(jnp.arange(N_CTX, dtype=jnp.int32)[None, :, None], owner_grid.shape)
    slot = column * (GROUPS * MOST) + source * MOST + page_rank
    target_group = owner_grid.reshape(-1)
    slot_flat = slot.reshape(-1)
    pool = jnp.zeros((GROUPS, POOL, 2, PAGE, E), jnp.bfloat16)
    pool = pool.at[target_group, slot_flat].set(stored.reshape(GROUPS * PAGES, 2, PAGE, E))
    pool_scales = jnp.zeros((GROUPS, POOL, 2), jnp.bfloat16)
    pool_scales = pool_scales.at[target_group, slot_flat].set(scales.reshape(GROUPS * PAGES, 2))
    return (attended, pool, pool_scales)
```

```python
import math

import jax
import jax.numpy as jnp
from jax import lax
from jax.experimental import pallas as pl
from jax.experimental.pallas import tpu as pltpu
from jax.sharding import PartitionSpec as P

E = 128
HQ = 32
HK = 4
PAGE = 128
T = 256
REP = HQ // HK
SIDE = 4
ROWS = T + 8
W = 4 * E
epsilon = 1e-06
exp2_scale = math.log2(math.e) / math.sqrt(E)
low = -1e30


def along_z(step):
    return [(SIDE * y + z, SIDE * y + (z + step) % SIDE) for y in range(SIDE) for z in range(SIDE)]


def along_y(step):
    return [(SIDE * y + z, SIDE * ((y + step) % SIDE) + z) for y in range(SIDE) for z in range(SIDE)]


def attend_stage(places, pieces, first, last):
    n_low, n_high = counts = tuple(len(half) for half in places)
    most = max(counts)

    def kernel(*refs):
        refs = list(refs)
        tab, start_ref, q_ref = refs[:3]
        del refs[:3]
        if not first:
            acc_in, m_in, l_in = refs[:3]
            del refs[:3]
        operands = []
        for half in range(2):
            operands.append(refs[: len(pieces[half])])
            del refs[: len(pieces[half])]
        if last:
            out_ref = refs.pop(0)
        else:
            acc_out, m_out, l_out = refs[:3]
            del refs[:3]
        kv = refs[:2]
        s_ref = refs[2:4]
        m_ref = refs[4:6]
        acc, l_ref, lists, sems = refs[6:]
        step = pl.program_id(0)
        starts = start_ref[0:1, :]
        in_first_doc = starts == 0
        lane = lax.broadcasted_iota(jnp.int32, (T, T), 1)
        row = lax.broadcasted_iota(jnp.int32, (T, T), 0)

        def scalars(half):
            return lists[half, 16], lists[half, 17], lists[half, 18], lists[half, 19]

        def load():
            copies = []
            for half in range(2):
                for k, (ref, (at, n)) in enumerate(zip(operands[half], pieces[half])):
                    copy = pltpu.make_async_copy(ref, kv[half].at[pl.ds(at, n)], sems.at[half, k])
                    copy.start()
                    copies.append(copy)
            for copy in copies:
                copy.wait()
            own = tab[0]
            doc = tab[1].astype(jnp.float32)
            y, z = lax.shift_right_logical(own, 2), own & 3
            for half in range(2):
                n = jnp.int32(0)
                has = jnp.int32(0)
                edge = jnp.int32(0)
                edge_row = jnp.int32(0)
                begin = 1 if first else 0
                for slot in range(begin, counts[half]):
                    ids = kv[half][slot, T : T + 8, 0:T].astype(jnp.float32)[0:1]
                    same = jnp.sum(jnp.where(ids == doc, 1.0, 0.0)).astype(jnp.int32)
                    dy, dz = places[half][slot]
                    chunk = ((y + dy) & 3) * SIDE + ((z + dz) & 3)
                    same = jnp.where(chunk < own, same, 0)
                    lists[half, n] = slot
                    n = n + jnp.where(same == T, 1, 0)
                    part = (same > 0) & (same < T)
                    has = jnp.where(part, 1, has)
                    edge = jnp.where(part, slot, edge)
                    edge_row = jnp.where(part, T - same, edge_row)
                lists[half, 16] = n
                lists[half, 17] = has
                lists[half, 18] = edge
                lists[half, 19] = edge_row

        def scores(g, slot, h):
            keys = kv[g // 2][slot, 0:T, pl.ds((g % 2) * E, E)]
            queries = q_ref[:, pl.ds(h * E, E)]
            return lax.dot_general(
                keys, queries, (((1,), (1,)), ((), ())), preferred_element_type=jnp.float32
            )

        def top(s):
            return jnp.max(s.reshape(T // 8, 8, T), axis=0)

        def keep(g, h, place, s):
            b = g % 2
            s_ref[b][h, pl.ds(place * T, T), :] = s
            m_ref[b][h] = jnp.maximum(m_ref[b][h], top(s))

        def weigh(g, h, place, slot, largest):
            p = jnp.exp2((s_ref[g % 2][h, pl.ds(place * T, T), :] - largest[h]) * exp2_scale)
            l_ref[h] += jnp.sum(p.reshape(T // 8, 8, T), axis=0)
            values = kv[g // 2][slot, 0:T, pl.ds((2 + g % 2) * E, E)]
            acc[h] += lax.dot_general(
                values, p.astype(jnp.bfloat16), (((0,), (0,)), ((), ())),
                preferred_element_type=jnp.float32,
            )

        def turn(score_g, weigh_g):
            if weigh_g is not None:
                b = weigh_g % 2
                largest = []
                for h in range(REP):
                    m = jnp.max(m_ref[b][h], axis=0, keepdims=True)
                    if first:
                        acc[h] = jnp.zeros((E, T), jnp.float32)
                        l_ref[h] = jnp.zeros((8, T), jnp.float32)
                    else:
                        before = m_in[h, 0:1]
                        m = jnp.maximum(before, jnp.where(in_first_doc, m, low))
                        shrink = jnp.exp2((before - m) * exp2_scale)
                        acc[h] = acc_in[h] * shrink
                        l_ref[h] = l_in[h] * shrink
                    if not last:
                        m_out[h] = jnp.broadcast_to(m, (8, T))
                    largest.append(m)
                prior = [jnp.where(in_first_doc, m, -low) for m in largest]
                n_w, has_w, edge_w, _ = scalars(weigh_g // 2)
            if score_g is not None:
                m_ref[score_g % 2][...] = jnp.full((REP, 8, T), low, jnp.float32)
                n_s, has_s, edge_s, edge_row = scalars(score_g // 2)

            def one_score(i, h):
                keep(score_g, h, 2 + i, scores(score_g, lists[score_g // 2, i], h))

            def one_weigh(i, h):
                weigh(weigh_g, h, 2 + i, lists[weigh_g // 2, i], prior)

            def edge_score(h):
                s = scores(score_g, edge_s, h)
                keep(score_g, h, 1, jnp.where(row >= edge_row, s, low))

            def edge_weigh(h):
                weigh(weigh_g, h, 1, edge_w, prior)

            def loop(begin, end, works):
                def body(i, _):
                    for h in range(REP):
                        for work in works:
                            work(i, h)
                    return 0

                lax.fori_loop(begin, end, body, 0)

            def e_score(i, h):
                edge_score(h)

            def e_weigh(i, h):
                edge_weigh(h)

            if score_g is None:
                loop(0, n_w, [one_weigh])
                loop(0, has_w, [e_weigh])
            elif weigh_g is None:
                loop(0, n_s, [one_score])
                loop(0, has_s, [e_score])
            elif score_g // 2 == weigh_g // 2:
                loop(0, n_s, [one_score, one_weigh])
                loop(0, has_s, [e_score, e_weigh])
            else:
                both = jnp.minimum(n_s, n_w)
                loop(0, both, [one_score, one_weigh])
                loop(both, n_s, [one_score])
                loop(both, n_w, [one_weigh])
                loop(0, has_s, [e_score])
                loop(0, has_w, [e_weigh])
            for h in range(REP):
                if first:
                    if score_g is not None:
                        b = score_g % 2
                        s = scores(score_g, 0, h)
                        s = jnp.where((row >= starts) & (row <= lane), s, low)
                        m_ref[b][h] = jnp.where(in_first_doc, m_ref[b][h], low)
                        keep(score_g, h, 0, s)
                    if weigh_g is not None:
                        weigh(weigh_g, h, 0, 0, largest)
                if weigh_g is not None:
                    if last:
                        total = jnp.sum(l_ref[h], axis=0, keepdims=True)
                        result = (acc[h] / total).astype(jnp.bfloat16)
                        out_ref[:, pl.ds(h * E, E)] = result.T
                    else:
                        acc_out[h] = acc[h]
                        l_out[h] = l_ref[h]

        for k in range(HK + 1):

            @pl.when(step == k)
            def _(k=k):
                if k == 0:
                    load()
                turn(k if k < HK else None, k - 1 if k > 0 else None)

    def now(i):
        return jnp.minimum(i, HK - 1)

    def behind(i):
        return jnp.maximum(i - 1, 0)

    carry_specs = [
        pl.BlockSpec((REP, E, T), lambda i: (behind(i), 0, 0)),
        pl.BlockSpec((REP, 8, T), lambda i: (behind(i), 0, 0)),
        pl.BlockSpec((REP, 8, T), lambda i: (behind(i), 0, 0)),
    ]
    carry_shapes = [
        jax.ShapeDtypeStruct((HQ, E, T), jnp.float32),
        jax.ShapeDtypeStruct((HQ, 8, T), jnp.float32),
        jax.ShapeDtypeStruct((HQ, 8, T), jnp.float32),
    ]
    in_specs = [
        pl.BlockSpec(memory_space=pltpu.SMEM),
        pl.BlockSpec((8, T), lambda i: (0, 0)),
        pl.BlockSpec((T, REP * E), lambda i: (0, now(i))),
    ]
    if not first:
        in_specs += carry_specs
    in_specs += [pl.BlockSpec(memory_space=pl.ANY)] * (len(pieces[0]) + len(pieces[1]))
    if last:
        out_specs = pl.BlockSpec((T, REP * E), lambda i: (0, behind(i)))
        out_shape = jax.ShapeDtypeStruct((T, HQ * E), jnp.bfloat16)
    else:
        out_specs, out_shape = carry_specs, carry_shapes
    work = (n_low + n_high) // 2 * T * T * E * HQ * 4
    return pl.pallas_call(
        kernel,
        grid=(HK + 1,),
        in_specs=in_specs,
        out_specs=out_specs,
        out_shape=out_shape,
        scratch_shapes=[
            pltpu.VMEM((n_low, ROWS, W), jnp.bfloat16),
            pltpu.VMEM((n_high, ROWS, W), jnp.bfloat16),
            pltpu.VMEM((REP, (most + 2) * T, T), jnp.float32),
            pltpu.VMEM((REP, (most + 2) * T, T), jnp.float32),
            pltpu.VMEM((REP, 8, T), jnp.float32),
            pltpu.VMEM((REP, 8, T), jnp.float32),
            pltpu.VMEM((REP, E, T), jnp.float32),
            pltpu.VMEM((REP, 8, T), jnp.float32),
            pltpu.SMEM((2, 32), jnp.int32),
            pltpu.SemaphoreType.DMA((2, 4)),
        ],
        compiler_params=pltpu.CompilerParams(
            dimension_semantics=("arbitrary",), vmem_limit_bytes=60000 * 1024
        ),
        cost_estimate=pl.CostEstimate(flops=work, transcendentals=0, bytes_accessed=1 << 22),
        name="attend_first" if first else "attend_last" if last else "attend_middle",
    )


def pack_pages(keys, values, owner_list):
    def kernel(owner_ref, k_ref, v_ref, out_ref):
        out_ref[...] = jnp.zeros(out_ref.shape, out_ref.dtype)
        lane = lax.broadcasted_iota(jnp.int32, (8, E), 1)
        for page in range(8):
            block, head = page // HK, page % HK
            owner = owner_ref[page]
            rank = jnp.int32(0)
            for other in range(page):
                rank = rank + jnp.where(owner_ref[other] == owner, 1, 0)
            slot = owner * 2 + jnp.minimum(rank, 1)
            scales = []
            for which, ref in enumerate((k_ref, v_ref)):
                x = ref[block * PAGE : (block + 1) * PAGE, head * E : (head + 1) * E]
                x = x.astype(jnp.float32)
                size = jnp.max(jnp.max(jnp.abs(x), axis=0, keepdims=True), axis=1, keepdims=True)
                scale = (size + epsilon).astype(jnp.bfloat16).astype(jnp.float32)
                out_ref[slot, which * PAGE : (which + 1) * PAGE, :] = (x / scale).astype(
                    jnp.bfloat16
                )
                scales.append(scale)
            both = jnp.where(lane == 0, scales[0], jnp.where(lane == 1, scales[1], 0.0))
            out_ref[slot, 2 * PAGE : 2 * PAGE + 8, :] = both.astype(jnp.bfloat16)

    return pl.pallas_call(
        kernel,
        in_specs=[
            pl.BlockSpec(memory_space=pltpu.SMEM),
            pl.BlockSpec(memory_space=pltpu.VMEM),
            pl.BlockSpec(memory_space=pltpu.VMEM),
        ],
        out_specs=pl.BlockSpec(memory_space=pltpu.VMEM),
        out_shape=jax.ShapeDtypeStruct((16, 2 * PAGE + 8, E), jnp.bfloat16),
        name="pack_pages",
    )(owner_list, keys, values)


def local(query_rows, key_rows, value_rows, documents, owners):
    queries, keys, values = query_rows[0], key_rows[0], value_rows[0]
    docs = documents[0]
    here = lax.axis_index("ctx")

    ids = jnp.pad(docs.astype(jnp.bfloat16)[None], ((0, 7), (0, W - T)))
    halves = [
        jnp.concatenate(
            [jnp.concatenate([keys[:, c : c + 2 * E], values[:, c : c + 2 * E]], axis=1), ids]
        )
        for c in (0, 2 * E)
    ]

    def send(x, pairs):
        return lax.ppermute(x, "ctx", pairs)

    def gather(x, along, cut):
        up, down = send(x, along(1)), send(x, along(-1))
        far_up, far_down = send(up[:cut], along(1)), send(down[cut:], along(-1))
        return up, down, far_up, far_down

    def chunks(x):
        return x.reshape(-1, ROWS, W)

    sets = [
        jnp.concatenate([x, *gather(x, along, PAGE)])
        for x, along in zip(halves, (along_z, along_y))
    ]
    low_set = [chunks(x) for x in gather(sets[0], along_y, 2 * ROWS)]
    high_set = [chunks(x) for x in gather(sets[1], along_z, 2 * ROWS)]

    steps = (0, -1, 1, 2)

    table = jnp.stack([here, docs[0]]).astype(jnp.int32)
    starts = jnp.sum((docs[:, None] < docs[None, :]).astype(jnp.int32), axis=0)
    starts = jnp.broadcast_to(starts[None], (8, T))

    carry = attend_stage(
        ([(0, d) for d in steps], [(d, 0) for d in steps]), (((0, 4),), ((0, 4),)), True, False
    )(table, starts, queries, chunks(sets[0]), chunks(sets[1]))
    carry = attend_stage(
        ([(s, d) for s in (-1, 1) for d in steps], [(d, s) for s in (-1, 1) for d in steps]),
        (((0, 4), (4, 4)), ((0, 4), (4, 4))), False, False,
    )(table, starts, queries, *carry, *low_set[:2], *high_set[:2])
    attended = attend_stage(
        ([(2, d) for d in steps], [(d, 2) for d in steps]),
        (((0, 2), (2, 2)), ((0, 2), (2, 2))), False, True,
    )(table, starts, queries, *carry, *low_set[2:], *high_set[2:])

    packed = pack_pages(keys, values, owners[0, :, 0])
    arrived = lax.all_to_all(
        packed.reshape(8, 2, 2 * PAGE + 8, E), "group", split_axis=0, concat_axis=0, tiled=True
    ).reshape(16, 2 * PAGE + 8, E)
    pool = arrived[:, : 2 * PAGE].reshape(1, 16, 2, PAGE, E)
    return attended[None], pool, arrived[None, :, 2 * PAGE, :2]


def solution(mesh):
    placed = (
        P("group", "ctx", None),
        P("group", "ctx", None),
        P("group", "ctx", None),
        P("group", "ctx"),
        P("group", "ctx", None),
    )
    return jax.shard_map(
        local,
        mesh=mesh,
        in_specs=placed,
        out_specs=(
            P("group", "ctx", None),
            P("group", "ctx", None, None, None),
            P("group", "ctx", None),
        ),
        check_vma=False,
    )
```

```python
import math

import jax
import jax.numpy as jnp
from jax import lax
from jax.experimental import pallas as pl
from jax.experimental.pallas import tpu as pltpu
from jax.sharding import PartitionSpec as P


E = 128
HQ = 32
HK = 4
PAGE = 128
T = 256
REP = HQ // HK
SIDE = 4
ROWS = T + 8
W = 2 * HK * E
epsilon = 1e-06
exp2_scale = math.log2(math.e) / math.sqrt(E)
low = -1e30


def toward(leading, step):
    pairs = []
    for group in range(8):
        for y in range(SIDE):
            for z in range(SIDE):
                if (group % 2 == 0) == leading:
                    to = SIDE * y + (z + step) % SIDE
                else:
                    to = SIDE * ((y + step) % SIDE) + z
                pairs.append((SIDE * SIDE * group + SIDE * y + z, SIDE * SIDE * group + to))
    return pairs


def attend_stage(places, first, last):
    count = len(places)

    def kernel(*refs):
        refs = list(refs)
        here_ref, doc_ref, start_ref, q_ref = refs[:4]
        del refs[:4]
        if not first:
            acc_in, m_in, l_in = refs[:3]
            del refs[:3]
        operands = refs[: count // 2]
        del refs[: count // 2]
        if last:
            out_ref = refs.pop(0)
        else:
            acc_out, m_out, l_out = refs[:3]
            del refs[:3]
        kv = refs[0]
        s_ref = refs[1:3]
        m_ref = refs[3:5]
        acc, l_ref, lists, sems = refs[5:]
        step = pl.program_id(0)
        starts = start_ref[0:1, :]
        in_first_doc = starts == 0
        lane = lax.broadcasted_iota(jnp.int32, (T, T), 1)
        row = lax.broadcasted_iota(jnp.int32, (T, T), 0)

        def load():
            copies = []
            for k, ref in enumerate(operands):
                copy = pltpu.make_async_copy(ref, kv.at[pl.ds(2 * k, 2)], sems.at[k])
                copy.start()
                copies.append(copy)
            for copy in copies:
                copy.wait()
            own = here_ref[0]
            swapped = here_ref[1] == 1
            doc = doc_ref[0].astype(jnp.float32)
            y, z = lax.shift_right_logical(own, 2), own & 3
            n = jnp.int32(0)
            has = jnp.int32(0)
            edge = jnp.int32(0)
            edge_row = jnp.int32(0)
            for slot in range(1 if first else 0, count):
                ids = kv[slot, T : T + 8, 0:T].astype(jnp.float32)[0:1]
                same = jnp.sum(jnp.where(ids == doc, 1.0, 0.0)).astype(jnp.int32)
                lead, follow = places[slot]
                dy = jnp.where(swapped, lead, follow)
                dz = jnp.where(swapped, follow, lead)
                chunk = ((y + dy) & 3) * SIDE + ((z + dz) & 3)
                same = jnp.where(chunk < own, same, 0)
                lists[n] = slot
                n = n + jnp.where(same == T, 1, 0)
                part = (same > 0) & (same < T)
                has = jnp.where(part, 1, has)
                edge = jnp.where(part, slot, edge)
                edge_row = jnp.where(part, T - same, edge_row)
            lists[16] = n
            lists[17] = has
            lists[18] = edge
            lists[19] = edge_row

        def scores(g, slot, h):
            keys = kv[slot, 0:T, pl.ds(pl.multiple_of(g * E, E), E)]
            queries = q_ref[:, pl.ds(h * E, E)]
            return lax.dot_general(
                keys, queries, (((1,), (1,)), ((), ())), preferred_element_type=jnp.float32
            )

        def top(s):
            return jnp.max(s.reshape(T // 8, 8, T), axis=0)

        def keep(b, h, place, s):
            s_ref[b][h, pl.ds(place * T, T), :] = s
            m_ref[b][h] = jnp.maximum(m_ref[b][h], top(s))

        def weigh(g, b, h, sources, largest):
            total, sums = None, None
            for place, slot in sources:
                p = jnp.exp2((s_ref[b][h, pl.ds(place * T, T), :] - largest[h]) * exp2_scale)
                part = jnp.sum(p.reshape(T // 8, 8, T), axis=0)
                values = kv[slot, 0:T, pl.ds(pl.multiple_of((HK + g) * E, E), E)]
                product = lax.dot_general(
                    values, p.astype(jnp.bfloat16), (((0,), (0,)), ((), ())),
                    preferred_element_type=jnp.float32,
                )
                total = product if total is None else total + product
                sums = part if sums is None else sums + part
            l_ref[h] += sums
            acc[h] += total

        def turn(scoring, weighing, b):
            score_g, weigh_g, a = step, step - 1, 1 - b
            n, has, edge, edge_row = lists[16], lists[17], lists[18], lists[19]
            if weighing:
                largest = []
                for h in range(REP):
                    m = jnp.max(m_ref[a][h], axis=0, keepdims=True)
                    if first:
                        acc[h] = jnp.zeros((E, T), jnp.float32)
                        l_ref[h] = jnp.zeros((8, T), jnp.float32)
                    else:
                        before = m_in[h, 0:1]
                        m = jnp.maximum(before, jnp.where(in_first_doc, m, low))
                        shrink = jnp.exp2((before - m) * exp2_scale)
                        acc[h] = acc_in[h] * shrink
                        l_ref[h] = l_in[h] * shrink
                    if not last:
                        m_out[h] = jnp.broadcast_to(m, (8, T))
                    largest.append(m)
                prior = [jnp.where(in_first_doc, m, -low) for m in largest]
            if scoring:
                m_ref[b][...] = jnp.full((REP, 8, T), low, jnp.float32)

            def whole(at, width):
                for h in range(REP):
                    if scoring:
                        for w in range(width):
                            keep(b, h, 2 + at + w, scores(score_g, lists[at + w], h))
                    if weighing:
                        sources = [(2 + at + w, lists[at + w]) for w in range(width)]
                        weigh(weigh_g, a, h, sources, prior)

            def pair(i, _):
                whole(2 * i, 2)
                return 0

            def single(i, _):
                whole(i, 1)
                return 0

            def cut(i, _):
                for h in range(REP):
                    if scoring:
                        s = scores(score_g, edge, h)
                        keep(b, h, 1, jnp.where(row >= edge_row, s, low))
                    if weighing:
                        weigh(weigh_g, a, h, [(1, edge)], prior)
                return 0

            pairs = lax.shift_right_logical(n, 1)
            lax.fori_loop(0, pairs, pair, 0)
            lax.fori_loop(2 * pairs, n, single, 0)
            lax.fori_loop(0, has, cut, 0)
            for h in range(REP):
                if first:
                    if scoring:
                        s = scores(score_g, 0, h)
                        s = jnp.where((row >= starts) & (row <= lane), s, low)
                        m_ref[b][h] = jnp.where(in_first_doc, m_ref[b][h], low)
                        keep(b, h, 0, s)
                    if weighing:
                        weigh(weigh_g, a, h, [(0, 0)], largest)
                if weighing:
                    if last:
                        total = jnp.sum(l_ref[h], axis=0, keepdims=True)
                        result = (acc[h] / total).astype(jnp.bfloat16)
                        out_ref[:, pl.ds(h * E, E)] = result.T
                    else:
                        acc_out[h] = acc[h]
                        l_out[h] = l_ref[h]

        @pl.when(step == 0)
        def _():
            load()
            turn(True, False, 0)

        @pl.when((step == 1) | (step == 3))
        def _():
            turn(True, True, 1)

        @pl.when(step == 2)
        def _():
            turn(True, True, 0)

        @pl.when(step == HK)
        def _():
            turn(False, True, 0)

    def now(i):
        return jnp.minimum(i, HK - 1)

    def behind(i):
        return jnp.maximum(i - 1, 0)

    carry_specs = [
        pl.BlockSpec((REP, E, T), lambda i: (behind(i), 0, 0)),
        pl.BlockSpec((REP, 8, T), lambda i: (behind(i), 0, 0)),
        pl.BlockSpec((REP, 8, T), lambda i: (behind(i), 0, 0)),
    ]
    carry_shapes = [
        jax.ShapeDtypeStruct((HQ, E, T), jnp.float32),
        jax.ShapeDtypeStruct((HQ, 8, T), jnp.float32),
        jax.ShapeDtypeStruct((HQ, 8, T), jnp.float32),
    ]
    in_specs = [
        pl.BlockSpec(memory_space=pltpu.SMEM),
        pl.BlockSpec(memory_space=pltpu.SMEM),
        pl.BlockSpec((8, T), lambda i: (0, 0)),
        pl.BlockSpec((T, REP * E), lambda i: (0, now(i))),
    ]
    if not first:
        in_specs += carry_specs
    in_specs += [pl.BlockSpec(memory_space=pl.ANY)] * (count // 2)
    if last:
        out_specs = pl.BlockSpec((T, REP * E), lambda i: (0, behind(i)))
        out_shape = jax.ShapeDtypeStruct((T, HQ * E), jnp.bfloat16)
    else:
        out_specs, out_shape = carry_specs, carry_shapes
    return pl.pallas_call(
        kernel,
        grid=(HK + 1,),
        in_specs=in_specs,
        out_specs=out_specs,
        out_shape=out_shape,
        scratch_shapes=[
            pltpu.VMEM((count, ROWS, W), jnp.bfloat16),
            pltpu.VMEM((REP, (count + 2) * T, T), jnp.float32),
            pltpu.VMEM((REP, (count + 2) * T, T), jnp.float32),
            pltpu.VMEM((REP, 8, T), jnp.float32),
            pltpu.VMEM((REP, 8, T), jnp.float32),
            pltpu.VMEM((REP, E, T), jnp.float32),
            pltpu.VMEM((REP, 8, T), jnp.float32),
            pltpu.SMEM((32,), jnp.int32),
            pltpu.SemaphoreType.DMA((4,)),
        ],
        compiler_params=pltpu.CompilerParams(
            dimension_semantics=("arbitrary",), vmem_limit_bytes=58 * 1024 * 1024
        ),
        cost_estimate=pl.CostEstimate(
            flops=count * T * T * E * HQ * 4, transcendentals=0, bytes_accessed=1 << 22
        ),
        name="attend_first" if first else "attend_last" if last else "attend_middle",
    )


def pack_pages(keys, values, owner_list):
    def kernel(owner_ref, k_ref, v_ref, out_ref):
        out_ref[...] = jnp.zeros(out_ref.shape, out_ref.dtype)
        lane = lax.broadcasted_iota(jnp.int32, (8, E), 1)
        for page in range(8):
            block, head = page // HK, page % HK
            owner = owner_ref[page]
            rank = jnp.int32(0)
            for other in range(page):
                rank = rank + jnp.where(owner_ref[other] == owner, 1, 0)
            slot = owner * 2 + jnp.minimum(rank, 1)
            scales = []
            for which, ref in enumerate((k_ref, v_ref)):
                x = ref[block * PAGE : (block + 1) * PAGE, head * E : (head + 1) * E]
                x = x.astype(jnp.float32)
                size = jnp.max(jnp.max(jnp.abs(x), axis=0, keepdims=True), axis=1, keepdims=True)
                scale = (size + epsilon).astype(jnp.bfloat16).astype(jnp.float32)
                out_ref[slot, which * PAGE : (which + 1) * PAGE, :] = (x / scale).astype(
                    jnp.bfloat16
                )
                scales.append(scale)
            both = jnp.where(lane == 0, scales[0], jnp.where(lane == 1, scales[1], 0.0))
            out_ref[slot, 2 * PAGE : 2 * PAGE + 8, :] = both.astype(jnp.bfloat16)

    return pl.pallas_call(
        kernel,
        in_specs=[
            pl.BlockSpec(memory_space=pltpu.SMEM),
            pl.BlockSpec(memory_space=pltpu.VMEM),
            pl.BlockSpec(memory_space=pltpu.VMEM),
        ],
        out_specs=pl.BlockSpec(memory_space=pltpu.VMEM),
        out_shape=jax.ShapeDtypeStruct((16, 2 * PAGE + 8, E), jnp.bfloat16),
        name="pack_pages",
    )(owner_list, keys, values)


def prepare(keys, values, docs):
    def kernel(k_ref, v_ref, doc_ref, chunk_ref, start_ref):
        docs = doc_ref[...]
        chunk_ref[0:T, 0 : HK * E] = k_ref[...]
        chunk_ref[0:T, HK * E : W] = v_ref[...]
        chunk_ref[T:ROWS, 0:T] = jnp.broadcast_to(docs.astype(jnp.float32), (8, T)).astype(
            jnp.bfloat16
        )
        chunk_ref[T:ROWS, T:W] = jnp.zeros((8, W - T), jnp.bfloat16)
        starts = jnp.zeros((1, T), jnp.int32)
        for doc in range(1, 4):
            before = jnp.sum(
                jnp.where(docs < doc, 1.0, 0.0), axis=1, keepdims=True
            ).astype(jnp.int32)
            starts = jnp.where(docs == doc, before, starts)
        start_ref[...] = jnp.broadcast_to(starts, (8, T))

    vmem = pl.BlockSpec(memory_space=pltpu.VMEM)
    return pl.pallas_call(
        kernel,
        in_specs=[vmem] * 3,
        out_specs=[vmem] * 2,
        out_shape=[
            jax.ShapeDtypeStruct((ROWS, W), jnp.bfloat16),
            jax.ShapeDtypeStruct((8, T), jnp.int32),
        ],
        name="prepare",
    )(keys, values, docs)


def whole_step(query_rows, key_rows, value_rows, documents, owners):
    queries, keys, values = query_rows[0], key_rows[0], value_rows[0]
    docs = documents[0]
    here = jnp.stack([lax.axis_index("ctx"), lax.axis_index("group") & 1]).astype(jnp.int32)

    def send(x, leading, step):
        return lax.ppermute(x, ("group", "ctx"), toward(leading, step))

    def chunks(x):
        return x.reshape(2, ROWS, W)

    own, starts = prepare(keys, values, documents)
    up, down = send(own, True, 1), send(own, True, -1)
    packed = pack_pages(keys, values, owners[0, :, 0])
    arrived = lax.all_to_all(
        packed.reshape(8, 2, 2 * PAGE + 8, E), "group", split_axis=0, concat_axis=0, tiled=True
    ).reshape(16, 2 * PAGE + 8, E)
    up, down, packed = lax.optimization_barrier((up, down, packed))
    far = send(up[:PAGE], True, 1), send(down[PAGE:], True, -1)
    one = jnp.concatenate([own, up])
    one_up = send(one, False, 1)
    two = jnp.concatenate([down, *far])
    two_down = send(two, False, -1)
    two_up, one_down = send(two, False, 1), send(one, False, -1)
    one_far, two_far = send(one_up, False, 1), send(two_down, False, -1)

    steps = (0, -1, 1, 2)
    common = (here, docs, starts, queries)
    carry = attend_stage([(d, 0) for d in steps], True, False)(*common, chunks(one), chunks(two))
    carry = attend_stage([(d, s) for s in (-1, 1) for d in steps], False, False)(
        *common, *carry, chunks(one_up), chunks(two_up), chunks(one_down), chunks(two_down)
    )
    attended = attend_stage([(d, 2) for d in steps], False, True)(
        *common, *carry, chunks(one_far), chunks(two_far)
    )

    pool = arrived[:, : 2 * PAGE].reshape(1, 16, 2, PAGE, E)
    return attended[None], pool, arrived[None, :, 2 * PAGE, :2]


def solution(mesh):
    placed = (
        P("group", "ctx", None),
        P("group", "ctx", None),
        P("group", "ctx", None),
        P("group", "ctx"),
        P("group", "ctx", None),
    )
    return jax.shard_map(
        whole_step,
        mesh=mesh,
        in_specs=placed,
        out_specs=(
            P("group", "ctx", None),
            P("group", "ctx", None, None, None),
            P("group", "ctx", None),
        ),
        check_vma=False,
    )
```

```python
import math

import jax
import jax.numpy as jnp
from jax import lax
from jax.experimental import pallas as pl
from jax.experimental.pallas import tpu as pltpu
from jax.sharding import PartitionSpec as P


E = 128
HQ = 32
HK = 4
PAGE = 128
T = 256
REP = HQ // HK
SIDE = 4
ROWS = T + 8
W = 2 * HK * E
epsilon = 1e-06
exp2_scale = math.log2(math.e) / math.sqrt(E)
low = -1e30


def toward(leading, step):
    pairs = []
    for group in range(8):
        for y in range(SIDE):
            for z in range(SIDE):
                if (group % 2 == 0) == leading:
                    to = SIDE * y + (z + step) % SIDE
                else:
                    to = SIDE * ((y + step) % SIDE) + z
                pairs.append((SIDE * SIDE * group + SIDE * y + z, SIDE * SIDE * group + to))
    return pairs


def attend_stage(places, pieces, first, last):
    count = len(places)

    def kernel(*refs):
        refs = list(refs)
        here_ref, doc_ref, start_ref, q_ref = refs[:4]
        del refs[:4]
        if not first:
            acc_in, m_in, l_in = refs[:3]
            del refs[:3]
        operands = refs[: len(pieces)]
        del refs[: len(pieces)]
        if last:
            out_ref = refs.pop(0)
        else:
            acc_out, m_out, l_out = refs[:3]
            del refs[:3]
        kv = refs[0]
        s_ref = refs[1:3]
        m_ref = refs[3:5]
        acc, l_ref, lists, sems = refs[5:]
        step = pl.program_id(0)
        starts = start_ref[0:1, :]
        in_first_doc = starts == 0
        lane = lax.broadcasted_iota(jnp.int32, (T, T), 1)
        row = lax.broadcasted_iota(jnp.int32, (T, T), 0)

        def load():
            copies = []
            at = 0
            for k, (ref, n) in enumerate(zip(operands, pieces)):
                copy = pltpu.make_async_copy(ref, kv.at[pl.ds(at, n)], sems.at[k])
                copy.start()
                copies.append(copy)
                at += n
            for copy in copies:
                copy.wait()
            own = here_ref[0]
            swapped = here_ref[1] == 1
            doc = doc_ref[0].astype(jnp.float32)
            y, z = lax.shift_right_logical(own, 2), own & 3
            n = jnp.int32(0)
            has = jnp.int32(0)
            edge = jnp.int32(0)
            edge_row = jnp.int32(0)
            for slot in range(1 if first else 0, count):
                ids = kv[slot, T : T + 8, 0:T].astype(jnp.float32)[0:1]
                same = jnp.sum(jnp.where(ids == doc, 1.0, 0.0)).astype(jnp.int32)
                lead, follow = places[slot]
                dy = jnp.where(swapped, lead, follow)
                dz = jnp.where(swapped, follow, lead)
                chunk = ((y + dy) & 3) * SIDE + ((z + dz) & 3)
                same = jnp.where(chunk < own, same, 0)
                lists[n] = slot
                n = n + jnp.where(same == T, 1, 0)
                part = (same > 0) & (same < T)
                has = jnp.where(part, 1, has)
                edge = jnp.where(part, slot, edge)
                edge_row = jnp.where(part, T - same, edge_row)
            lists[16] = n
            lists[17] = has
            lists[18] = edge
            lists[19] = edge_row

        def scores(g, slot, h):
            keys = kv[slot, 0:T, pl.ds(pl.multiple_of(g * E, E), E)]
            queries = q_ref[:, pl.ds(h * E, E)]
            return lax.dot_general(
                keys, queries, (((1,), (1,)), ((), ())), preferred_element_type=jnp.float32
            )

        def top(s):
            return jnp.max(s.reshape(T // 8, 8, T), axis=0)

        def keep(b, h, place, s):
            s_ref[b][h, pl.ds(place * T, T), :] = s
            m_ref[b][h] = jnp.maximum(m_ref[b][h], top(s))

        def weigh(g, b, h, sources, largest):
            total, sums = None, None
            for place, slot in sources:
                p = jnp.exp2((s_ref[b][h, pl.ds(place * T, T), :] - largest[h]) * exp2_scale)
                part = jnp.sum(p.reshape(T // 8, 8, T), axis=0)
                at = pl.multiple_of(lax.shift_right_logical(g, 1) * E, E)
                values = kv[slot, pl.ds(at, E), pl.ds(pl.multiple_of(HK * E + (g & 1) * T, T), T)]
                product = lax.dot_general(
                    values, p.astype(jnp.bfloat16), (((1,), (0,)), ((), ())),
                    preferred_element_type=jnp.float32,
                )
                total = product if total is None else total + product
                sums = part if sums is None else sums + part
            l_ref[h] += sums
            acc[h] += total

        def turn(scoring, weighing, b):
            score_g, weigh_g, a = step, step - 1, 1 - b
            n, has, edge, edge_row = lists[16], lists[17], lists[18], lists[19]
            if weighing:
                largest = []
                for h in range(REP):
                    m = jnp.max(m_ref[a][h], axis=0, keepdims=True)
                    if first:
                        acc[h] = jnp.zeros((E, T), jnp.float32)
                        l_ref[h] = jnp.zeros((8, T), jnp.float32)
                    else:
                        before = m_in[h, 0:1]
                        m = jnp.maximum(before, jnp.where(in_first_doc, m, low))
                        shrink = jnp.exp2((before - m) * exp2_scale)
                        acc[h] = acc_in[h] * shrink
                        l_ref[h] = l_in[h] * shrink
                    if not last:
                        m_out[h] = jnp.broadcast_to(m, (8, T))
                    largest.append(m)
                prior = [jnp.where(in_first_doc, m, -low) for m in largest]
            if scoring:
                m_ref[b][...] = jnp.full((REP, 8, T), low, jnp.float32)

            def whole(at, width):
                for h in range(REP):
                    if scoring:
                        for w in range(width):
                            keep(b, h, 2 + at + w, scores(score_g, lists[at + w], h))
                    if weighing:
                        sources = [(2 + at + w, lists[at + w]) for w in range(width)]
                        weigh(weigh_g, a, h, sources, prior)

            def pair(i, _):
                whole(2 * i, 2)
                return 0

            def single(i, _):
                whole(i, 1)
                return 0

            def cut(i, _):
                for h in range(REP):
                    if scoring:
                        s = scores(score_g, edge, h)
                        keep(b, h, 1, jnp.where(row >= edge_row, s, low))
                    if weighing:
                        weigh(weigh_g, a, h, [(1, edge)], prior)
                return 0

            pairs = lax.shift_right_logical(n, 1)
            lax.fori_loop(0, pairs, pair, 0)
            lax.fori_loop(2 * pairs, n, single, 0)
            lax.fori_loop(0, has, cut, 0)
            for h in range(REP):
                if first:
                    if scoring:
                        s = scores(score_g, 0, h)
                        s = jnp.where((row >= starts) & (row <= lane), s, low)
                        m_ref[b][h] = jnp.where(in_first_doc, m_ref[b][h], low)
                        keep(b, h, 0, s)
                    if weighing:
                        weigh(weigh_g, a, h, [(0, 0)], largest)
                if weighing:
                    if last:
                        total = jnp.sum(l_ref[h], axis=0, keepdims=True)
                        result = (acc[h] / total).astype(jnp.bfloat16)
                        out_ref[:, pl.ds(h * E, E)] = result.T
                    else:
                        acc_out[h] = acc[h]
                        l_out[h] = l_ref[h]

        @pl.when(step == 0)
        def _():
            load()
            turn(True, False, 0)

        @pl.when((step == 1) | (step == 3))
        def _():
            turn(True, True, 1)

        @pl.when(step == 2)
        def _():
            turn(True, True, 0)

        @pl.when(step == HK)
        def _():
            turn(False, True, 0)

    def now(i):
        return jnp.minimum(i, HK - 1)

    def behind(i):
        return jnp.maximum(i - 1, 0)

    carry_specs = [
        pl.BlockSpec((REP, E, T), lambda i: (behind(i), 0, 0)),
        pl.BlockSpec((REP, 8, T), lambda i: (behind(i), 0, 0)),
        pl.BlockSpec((REP, 8, T), lambda i: (behind(i), 0, 0)),
    ]
    carry_shapes = [
        jax.ShapeDtypeStruct((HQ, E, T), jnp.float32),
        jax.ShapeDtypeStruct((HQ, 8, T), jnp.float32),
        jax.ShapeDtypeStruct((HQ, 8, T), jnp.float32),
    ]
    in_specs = [
        pl.BlockSpec(memory_space=pltpu.SMEM),
        pl.BlockSpec(memory_space=pltpu.SMEM),
        pl.BlockSpec((8, T), lambda i: (0, 0)),
        pl.BlockSpec((T, REP * E), lambda i: (0, now(i))),
    ]
    if not first:
        in_specs += carry_specs
    in_specs += [pl.BlockSpec(memory_space=pl.ANY)] * len(pieces)
    if last:
        out_specs = pl.BlockSpec((T, REP * E), lambda i: (0, behind(i)))
        out_shape = jax.ShapeDtypeStruct((T, HQ * E), jnp.bfloat16)
    else:
        out_specs, out_shape = carry_specs, carry_shapes
    return pl.pallas_call(
        kernel,
        grid=(HK + 1,),
        in_specs=in_specs,
        out_specs=out_specs,
        out_shape=out_shape,
        scratch_shapes=[
            pltpu.VMEM((count, ROWS, W), jnp.bfloat16),
            pltpu.VMEM((REP, (count + 2) * T, T), jnp.float32),
            pltpu.VMEM((REP, (count + 2) * T, T), jnp.float32),
            pltpu.VMEM((REP, 8, T), jnp.float32),
            pltpu.VMEM((REP, 8, T), jnp.float32),
            pltpu.VMEM((REP, E, T), jnp.float32),
            pltpu.VMEM((REP, 8, T), jnp.float32),
            pltpu.SMEM((32,), jnp.int32),
            pltpu.SemaphoreType.DMA((len(pieces),)),
        ],
        compiler_params=pltpu.CompilerParams(
            dimension_semantics=("arbitrary",), vmem_limit_bytes=58 * 1024 * 1024
        ),
        cost_estimate=pl.CostEstimate(
            flops=count * T * T * E * HQ * 4, transcendentals=0, bytes_accessed=1 << 22
        ),
        name="attend_first" if first else "attend_last" if last else "attend_middle",
    )


def pack_pages(keys, values, owner_list):
    def kernel(owner_ref, k_ref, v_ref, out_ref):
        out_ref[...] = jnp.zeros(out_ref.shape, out_ref.dtype)
        lane = lax.broadcasted_iota(jnp.int32, (8, E), 1)
        for page in range(8):
            block, head = page // HK, page % HK
            owner = owner_ref[page]
            rank = jnp.int32(0)
            for other in range(page):
                rank = rank + jnp.where(owner_ref[other] == owner, 1, 0)
            slot = owner * 2 + jnp.minimum(rank, 1)
            scales = []
            for which, ref in enumerate((k_ref, v_ref)):
                x = ref[block * PAGE : (block + 1) * PAGE, head * E : (head + 1) * E]
                x = x.astype(jnp.float32)
                size = jnp.max(jnp.max(jnp.abs(x), axis=0, keepdims=True), axis=1, keepdims=True)
                scale = (size + epsilon).astype(jnp.bfloat16).astype(jnp.float32)
                out_ref[slot, which * PAGE : (which + 1) * PAGE, :] = (x / scale).astype(
                    jnp.bfloat16
                )
                scales.append(scale)
            both = jnp.where(lane == 0, scales[0], jnp.where(lane == 1, scales[1], 0.0))
            out_ref[slot, 2 * PAGE : 2 * PAGE + 8, :] = both.astype(jnp.bfloat16)

    return pl.pallas_call(
        kernel,
        in_specs=[
            pl.BlockSpec(memory_space=pltpu.SMEM),
            pl.BlockSpec(memory_space=pltpu.VMEM),
            pl.BlockSpec(memory_space=pltpu.VMEM),
        ],
        out_specs=pl.BlockSpec(memory_space=pltpu.VMEM),
        out_shape=jax.ShapeDtypeStruct((16, 2 * PAGE + 8, E), jnp.bfloat16),
        name="pack_pages",
    )(owner_list, keys, values)


def prepare(keys, values, docs):
    def kernel(k_ref, v_ref, doc_ref, chunk_ref, start_ref):
        docs = doc_ref[...]
        chunk_ref[0:T, 0 : HK * E] = k_ref[...]
        for g in range(HK):
            at, lane = g // 2 * E, HK * E + g % 2 * T
            chunk_ref[at : at + E, lane : lane + T] = v_ref[:, g * E : (g + 1) * E].T
        chunk_ref[T:ROWS, 0:T] = jnp.broadcast_to(docs.astype(jnp.float32), (8, T)).astype(
            jnp.bfloat16
        )
        chunk_ref[T:ROWS, T:W] = jnp.zeros((8, W - T), jnp.bfloat16)
        starts = jnp.zeros((1, T), jnp.int32)
        for doc in range(1, 4):
            before = jnp.sum(
                jnp.where(docs < doc, 1.0, 0.0), axis=1, keepdims=True
            ).astype(jnp.int32)
            starts = jnp.where(docs == doc, before, starts)
        start_ref[...] = jnp.broadcast_to(starts, (8, T))

    vmem = pl.BlockSpec(memory_space=pltpu.VMEM)
    return pl.pallas_call(
        kernel,
        in_specs=[vmem] * 3,
        out_specs=[vmem] * 2,
        out_shape=[
            jax.ShapeDtypeStruct((ROWS, W), jnp.bfloat16),
            jax.ShapeDtypeStruct((8, T), jnp.int32),
        ],
        name="prepare",
    )(keys, values, docs)


def whole_step(query_rows, key_rows, value_rows, documents, owners):
    queries, keys, values = query_rows[0], key_rows[0], value_rows[0]
    docs = documents[0]
    here = jnp.stack([lax.axis_index("ctx"), lax.axis_index("group") & 1]).astype(jnp.int32)

    def send(x, leading, step):
        return lax.ppermute(x, ("group", "ctx"), toward(leading, step))

    def chunks(x):
        return x.reshape(-1, ROWS, W)

    own, starts = prepare(keys, values, documents)
    up, down = send(own, True, 1), send(own, True, -1)
    far = send(own, True, 2)
    own_up, own_down = send(own, False, 1), send(own, False, -1)
    packed = pack_pages(keys, values, owners[0, :, 0])
    arrived = lax.all_to_all(
        packed.reshape(8, 2, 2 * PAGE + 8, E), "group", split_axis=0, concat_axis=0, tiled=True
    ).reshape(16, 2 * PAGE + 8, E)
    up, down, packed = lax.optimization_barrier((up, down, packed))
    up_up, up_down = send(up, False, 1), send(up, False, -1)
    two = jnp.concatenate([down, far])
    two_down, two_up = send(two, False, -1), send(two, False, 1)
    own_far = send(own_up, False, 1)
    up_far = send(up_up, False, 1)
    two_far = send(two_down, False, -1)

    steps = (0, -1, 1, 2)
    common = (here, docs, starts, queries)

    def stage(follows, first, last, carry, operands):
        places = [(d, s) for s in follows for d in steps]
        pieces = (1, 1, 2) * len(follows)
        return attend_stage(places, pieces, first, last)(*common, *carry, *map(chunks, operands))

    carry = stage((0,), True, False, (), (own, up, two))
    carry = stage(
        (-1, 1), False, False, carry, (own_up, up_up, two_up, own_down, up_down, two_down)
    )
    attended = stage((2,), False, True, carry, (own_far, up_far, two_far))

    pool = arrived[:, : 2 * PAGE].reshape(1, 16, 2, PAGE, E)
    return attended[None], pool, arrived[None, :, 2 * PAGE, :2]


def solution(mesh):
    placed = (
        P("group", "ctx", None),
        P("group", "ctx", None),
        P("group", "ctx", None),
        P("group", "ctx"),
        P("group", "ctx", None),
    )
    return jax.shard_map(
        whole_step,
        mesh=mesh,
        in_specs=placed,
        out_specs=(
            P("group", "ctx", None),
            P("group", "ctx", None, None, None),
            P("group", "ctx", None),
        ),
        check_vma=False,
    )
```

```python
import math

import jax
import jax.numpy as jnp
from jax import lax
from jax.experimental import pallas as pl
from jax.experimental.pallas import tpu as pltpu
from jax.sharding import PartitionSpec as P


E = 128
HQ = 32
HK = 4
PAGE = 128
T = 256
REP = HQ // HK
SIDE = 4
ROWS = T + 8
W = 2 * HK * E
epsilon = 1e-06
exp2_scale = math.log2(math.e) / math.sqrt(E)
low = -1e30


def toward(leading, step):
    pairs = []
    for group in range(8):
        for y in range(SIDE):
            for z in range(SIDE):
                if (group % 2 == 0) == leading:
                    to = SIDE * y + (z + step) % SIDE
                else:
                    to = SIDE * ((y + step) % SIDE) + z
                pairs.append((SIDE * SIDE * group + SIDE * y + z, SIDE * SIDE * group + to))
    return pairs


def attend_stage(places, pieces, first, last):
    count = len(places)

    def kernel(*refs):
        refs = list(refs)
        here_ref, doc_ref, start_ref, q_ref = refs[:4]
        del refs[:4]
        if not first:
            acc_in, m_in, l_in = refs[:3]
            del refs[:3]
        operands = refs[: len(pieces)]
        del refs[: len(pieces)]
        if last:
            out_ref = refs.pop(0)
        else:
            acc_out, m_out, l_out = refs[:3]
            del refs[:3]
        kv = refs[0]
        s_ref = refs[1:3]
        m_ref = refs[3:5]
        acc, l_ref, lists, sems = refs[5:]
        step = pl.program_id(0)
        starts = start_ref[0:1, :]
        in_first_doc = starts == 0
        lane = lax.broadcasted_iota(jnp.int32, (T, T), 1)
        row = lax.broadcasted_iota(jnp.int32, (T, T), 0)

        def copies(part):
            at = 0
            result = []
            lanes = pl.ds(part * HK * E, HK * E)
            for k, (ref, n) in enumerate(zip(operands, pieces)):
                result.append(
                    pltpu.make_async_copy(
                        ref.at[:, :, lanes], kv.at[pl.ds(at, n), :, lanes], sems.at[part, k]
                    )
                )
                at += n
            return result

        def load():
            for part in range(2):
                for copy in copies(part):
                    copy.start()
            for copy in copies(0):
                copy.wait()
            own = here_ref[0]
            swapped = here_ref[1] == 1
            doc = doc_ref[0].astype(jnp.float32)
            y, z = lax.shift_right_logical(own, 2), own & 3
            n = jnp.int32(0)
            has = jnp.int32(0)
            edge = jnp.int32(0)
            edge_row = jnp.int32(0)
            for slot in range(1 if first else 0, count):
                ids = kv[slot, T : T + 8, 0:T].astype(jnp.float32)[0:1]
                same = jnp.sum(jnp.where(ids == doc, 1.0, 0.0)).astype(jnp.int32)
                lead, follow = places[slot]
                dy = jnp.where(swapped, lead, follow)
                dz = jnp.where(swapped, follow, lead)
                chunk = ((y + dy) & 3) * SIDE + ((z + dz) & 3)
                same = jnp.where(chunk < own, same, 0)
                lists[n] = slot
                n = n + jnp.where(same == T, 1, 0)
                part = (same > 0) & (same < T)
                has = jnp.where(part, 1, has)
                edge = jnp.where(part, slot, edge)
                edge_row = jnp.where(part, T - same, edge_row)
            lists[16] = n
            lists[17] = has
            lists[18] = edge
            lists[19] = edge_row

        def scores(g, slot, h):
            keys = kv[slot, 0:T, pl.ds(pl.multiple_of(g * E, E), E)]
            queries = q_ref[:, pl.ds(h * E, E)]
            return lax.dot_general(
                keys, queries, (((1,), (1,)), ((), ())), preferred_element_type=jnp.float32
            )

        def top(s):
            return jnp.max(s.reshape(T // 8, 8, T), axis=0)

        def keep(b, h, place, s):
            s_ref[b][h, pl.ds(place * T, T), :] = s
            m_ref[b][h] = jnp.maximum(m_ref[b][h], top(s))

        def weigh(g, b, h, sources, largest):
            total, sums = None, None
            for place, slot in sources:
                p = jnp.exp2((s_ref[b][h, pl.ds(place * T, T), :] - largest[h]) * exp2_scale)
                part = jnp.sum(p.reshape(T // 8, 8, T), axis=0)
                at = pl.multiple_of(lax.shift_right_logical(g, 1) * E, E)
                values = kv[slot, pl.ds(at, E), pl.ds(pl.multiple_of(HK * E + (g & 1) * T, T), T)]
                product = lax.dot_general(
                    values, p.astype(jnp.bfloat16), (((1,), (0,)), ((), ())),
                    preferred_element_type=jnp.float32,
                )
                total = product if total is None else total + product
                sums = part if sums is None else sums + part
            l_ref[h] += sums
            acc[h] += total

        def turn(scoring, weighing, b):
            score_g, weigh_g, a = step, step - 1, 1 - b
            n, has, edge, edge_row = lists[16], lists[17], lists[18], lists[19]
            if weighing:
                largest = []
                for h in range(REP):
                    m = jnp.max(m_ref[a][h], axis=0, keepdims=True)
                    if first:
                        acc[h] = jnp.zeros((E, T), jnp.float32)
                        l_ref[h] = jnp.zeros((8, T), jnp.float32)
                    else:
                        before = m_in[h, 0:1]
                        m = jnp.maximum(before, jnp.where(in_first_doc, m, low))
                        shrink = jnp.exp2((before - m) * exp2_scale)
                        acc[h] = acc_in[h] * shrink
                        l_ref[h] = l_in[h] * shrink
                    if not last:
                        m_out[h] = jnp.broadcast_to(m, (8, T))
                    largest.append(m)
                prior = [jnp.where(in_first_doc, m, -low) for m in largest]
            if scoring:
                m_ref[b][...] = jnp.full((REP, 8, T), low, jnp.float32)

            def whole(at, width):
                for h in range(REP):
                    if scoring:
                        for w in range(width):
                            keep(b, h, 2 + at + w, scores(score_g, lists[at + w], h))
                    if weighing:
                        sources = [(2 + at + w, lists[at + w]) for w in range(width)]
                        weigh(weigh_g, a, h, sources, prior)

            def pair(i, _):
                whole(2 * i, 2)
                return 0

            def single(i, _):
                whole(i, 1)
                return 0

            def cut(i, _):
                for h in range(REP):
                    if scoring:
                        s = scores(score_g, edge, h)
                        keep(b, h, 1, jnp.where(row >= edge_row, s, low))
                    if weighing:
                        weigh(weigh_g, a, h, [(1, edge)], prior)
                return 0

            pairs = lax.shift_right_logical(n, 1)
            lax.fori_loop(0, pairs, pair, 0)
            lax.fori_loop(2 * pairs, n, single, 0)
            lax.fori_loop(0, has, cut, 0)
            for h in range(REP):
                if first:
                    if scoring:
                        s = scores(score_g, 0, h)
                        s = jnp.where((row >= starts) & (row <= lane), s, low)
                        m_ref[b][h] = jnp.where(in_first_doc, m_ref[b][h], low)
                        keep(b, h, 0, s)
                    if weighing:
                        weigh(weigh_g, a, h, [(0, 0)], largest)
                if weighing:
                    if last:
                        total = jnp.sum(l_ref[h], axis=0, keepdims=True)
                        result = (acc[h] / total).astype(jnp.bfloat16)
                        out_ref[:, pl.ds(h * E, E)] = result.T
                    else:
                        acc_out[h] = acc[h]
                        l_out[h] = l_ref[h]

        @pl.when(step == 0)
        def _():
            load()
            turn(True, False, 0)

        @pl.when(step == 1)
        def _():
            for copy in copies(1):
                copy.wait()

        @pl.when((step == 1) | (step == 3))
        def _():
            turn(True, True, 1)

        @pl.when(step == 2)
        def _():
            turn(True, True, 0)

        @pl.when(step == HK)
        def _():
            turn(False, True, 0)

    def now(i):
        return jnp.minimum(i, HK - 1)

    def behind(i):
        return jnp.maximum(i - 1, 0)

    carry_specs = [
        pl.BlockSpec((REP, E, T), lambda i: (behind(i), 0, 0)),
        pl.BlockSpec((REP, 8, T), lambda i: (behind(i), 0, 0)),
        pl.BlockSpec((REP, 8, T), lambda i: (behind(i), 0, 0)),
    ]
    carry_shapes = [
        jax.ShapeDtypeStruct((HQ, E, T), jnp.float32),
        jax.ShapeDtypeStruct((HQ, 8, T), jnp.float32),
        jax.ShapeDtypeStruct((HQ, 8, T), jnp.float32),
    ]
    in_specs = [
        pl.BlockSpec(memory_space=pltpu.SMEM),
        pl.BlockSpec(memory_space=pltpu.SMEM),
        pl.BlockSpec((8, T), lambda i: (0, 0)),
        pl.BlockSpec((T, REP * E), lambda i: (0, now(i))),
    ]
    if not first:
        in_specs += carry_specs
    in_specs += [pl.BlockSpec(memory_space=pl.ANY)] * len(pieces)
    if last:
        out_specs = pl.BlockSpec((T, REP * E), lambda i: (0, behind(i)))
        out_shape = jax.ShapeDtypeStruct((T, HQ * E), jnp.bfloat16)
    else:
        out_specs, out_shape = carry_specs, carry_shapes
    return pl.pallas_call(
        kernel,
        grid=(HK + 1,),
        in_specs=in_specs,
        out_specs=out_specs,
        out_shape=out_shape,
        scratch_shapes=[
            pltpu.VMEM((count, ROWS, W), jnp.bfloat16),
            pltpu.VMEM((REP, (count + 2) * T, T), jnp.float32),
            pltpu.VMEM((REP, (count + 2) * T, T), jnp.float32),
            pltpu.VMEM((REP, 8, T), jnp.float32),
            pltpu.VMEM((REP, 8, T), jnp.float32),
            pltpu.VMEM((REP, E, T), jnp.float32),
            pltpu.VMEM((REP, 8, T), jnp.float32),
            pltpu.SMEM((32,), jnp.int32),
            pltpu.SemaphoreType.DMA((2, len(pieces))),
        ],
        compiler_params=pltpu.CompilerParams(
            dimension_semantics=("arbitrary",), vmem_limit_bytes=58 * 1024 * 1024
        ),
        cost_estimate=pl.CostEstimate(
            flops=count * T * T * E * HQ * 4, transcendentals=0, bytes_accessed=1 << 22
        ),
        name="attend_first" if first else "attend_last" if last else "attend_middle",
    )


def pack_pages(keys, values, owner_list):
    def kernel(owner_ref, k_ref, v_ref, out_ref):
        out_ref[...] = jnp.zeros(out_ref.shape, out_ref.dtype)
        lane = lax.broadcasted_iota(jnp.int32, (8, E), 1)
        for page in range(8):
            block, head = page // HK, page % HK
            owner = owner_ref[page]
            rank = jnp.int32(0)
            for other in range(page):
                rank = rank + jnp.where(owner_ref[other] == owner, 1, 0)
            slot = owner * 2 + jnp.minimum(rank, 1)
            scales = []
            for which, ref in enumerate((k_ref, v_ref)):
                x = ref[block * PAGE : (block + 1) * PAGE, head * E : (head + 1) * E]
                x = x.astype(jnp.float32)
                size = jnp.max(jnp.max(jnp.abs(x), axis=0, keepdims=True), axis=1, keepdims=True)
                scale = (size + epsilon).astype(jnp.bfloat16).astype(jnp.float32)
                out_ref[slot, which * PAGE : (which + 1) * PAGE, :] = (x / scale).astype(
                    jnp.bfloat16
                )
                scales.append(scale)
            both = jnp.where(lane == 0, scales[0], jnp.where(lane == 1, scales[1], 0.0))
            out_ref[slot, 2 * PAGE : 2 * PAGE + 8, :] = both.astype(jnp.bfloat16)

    return pl.pallas_call(
        kernel,
        in_specs=[
            pl.BlockSpec(memory_space=pltpu.SMEM),
            pl.BlockSpec(memory_space=pltpu.VMEM),
            pl.BlockSpec(memory_space=pltpu.VMEM),
        ],
        out_specs=pl.BlockSpec(memory_space=pltpu.VMEM),
        out_shape=jax.ShapeDtypeStruct((16, 2 * PAGE + 8, E), jnp.bfloat16),
        name="pack_pages",
    )(owner_list, keys, values)


def prepare(keys, values, docs):
    def kernel(k_ref, v_ref, doc_ref, chunk_ref, start_ref):
        docs = doc_ref[...]
        chunk_ref[0:T, 0 : HK * E] = k_ref[...]
        for g in range(HK):
            at, lane = g // 2 * E, HK * E + g % 2 * T
            chunk_ref[at : at + E, lane : lane + T] = v_ref[:, g * E : (g + 1) * E].T
        chunk_ref[T:ROWS, 0:T] = jnp.broadcast_to(docs.astype(jnp.float32), (8, T)).astype(
            jnp.bfloat16
        )
        chunk_ref[T:ROWS, T:W] = jnp.zeros((8, W - T), jnp.bfloat16)
        starts = jnp.zeros((1, T), jnp.int32)
        for doc in range(1, 4):
            before = jnp.sum(
                jnp.where(docs < doc, 1.0, 0.0), axis=1, keepdims=True
            ).astype(jnp.int32)
            starts = jnp.where(docs == doc, before, starts)
        start_ref[...] = jnp.broadcast_to(starts, (8, T))

    vmem = pl.BlockSpec(memory_space=pltpu.VMEM)
    return pl.pallas_call(
        kernel,
        in_specs=[vmem] * 3,
        out_specs=[vmem] * 2,
        out_shape=[
            jax.ShapeDtypeStruct((ROWS, W), jnp.bfloat16),
            jax.ShapeDtypeStruct((8, T), jnp.int32),
        ],
        name="prepare",
    )(keys, values, docs)


def whole_step(query_rows, key_rows, value_rows, documents, owners):
    queries, keys, values = query_rows[0], key_rows[0], value_rows[0]
    docs = documents[0]
    here = jnp.stack([lax.axis_index("ctx"), lax.axis_index("group") & 1]).astype(jnp.int32)

    def send(x, leading, step):
        return lax.ppermute(x, ("group", "ctx"), toward(leading, step))

    def chunks(x):
        return x.reshape(-1, ROWS, W)

    own, starts = prepare(keys, values, documents)
    up, down = send(own, True, 1), send(own, True, -1)
    own_up, own_down = send(own, False, 1), send(own, False, -1)
    packed = pack_pages(keys, values, owners[0, :, 0])
    arrived = lax.all_to_all(
        packed.reshape(8, 2, 2 * PAGE + 8, E), "group", split_axis=0, concat_axis=0, tiled=True
    ).reshape(16, 2 * PAGE + 8, E)
    up, down, packed = lax.optimization_barrier((up, down, packed))
    far = send(up[:PAGE], True, 1), send(down[PAGE:], True, -1)
    up_up, up_down = send(up, False, 1), send(up, False, -1)
    two = jnp.concatenate([down, *far])
    two_down, two_up = send(two, False, -1), send(two, False, 1)
    own_far = send(own_up, False, 1)
    up_far = send(up_up, False, 1)
    two_far = send(two_down, False, -1)

    steps = (0, -1, 1, 2)
    common = (here, docs, starts, queries)

    def stage(follows, first, last, carry, operands):
        places = [(d, s) for s in follows for d in steps]
        pieces = (1, 1, 2) * len(follows)
        return attend_stage(places, pieces, first, last)(*common, *carry, *map(chunks, operands))

    carry = stage((0,), True, False, (), (own, up, two))
    carry = stage(
        (-1, 1), False, False, carry, (own_up, up_up, two_up, own_down, up_down, two_down)
    )
    attended = stage((2,), False, True, carry, (own_far, up_far, two_far))

    pool = arrived[:, : 2 * PAGE].reshape(1, 16, 2, PAGE, E)
    return attended[None], pool, arrived[None, :, 2 * PAGE, :2]


def solution(mesh):
    placed = (
        P("group", "ctx", None),
        P("group", "ctx", None),
        P("group", "ctx", None),
        P("group", "ctx"),
        P("group", "ctx", None),
    )
    return jax.shard_map(
        whole_step,
        mesh=mesh,
        in_specs=placed,
        out_specs=(
            P("group", "ctx", None),
            P("group", "ctx", None, None, None),
            P("group", "ctx", None),
        ),
        check_vma=False,
    )
```
